32 devices in a mesh: wide: 8 (over z, x), narrow: 4 (over y, core).
Axes of the slice: x: 2, y: 2, z: 4, core: 2. Of those that a mesh axis runs over, the one named last changes fastest.
Arguments:
- tokens: bfloat16 [64, 256, 512], P(('wide', 'narrow')), may hold values from -6 to 6
- cotangent: bfloat16 [64, 256, 512], P(('wide', 'narrow')), may hold values from -0.29882812 to 0.29882812
- lengths: int32 [64], P(('wide', 'narrow')), may hold values from 160 to 256, as said below
- item_rows: int32 [64, 256], P(('wide', 'narrow')), may hold values from 0 to 1023, as said below
- w_in: bfloat16 [512, 2048], replicated, may hold values from -0.25 to 0.25
- w_out: bfloat16 [512, 512], replicated, may hold values from -0.25 to 0.25
- table: float32 [1024, 512], P(('wide', 'narrow')), may hold values from -6 to 6
- moment_one: float32 [1024, 512], P(('wide', 'narrow')), may hold values from -0.3 to 0.3
- moment_two: float32 [1024, 512], P(('wide', 'narrow')), may hold values from 0.0001 to 0.01
Outputs:
- table_new: float32 [1024, 512], P(('wide', 'narrow'))
- moment_one_new: float32 [1024, 512], P(('wide', 'narrow'))
- moment_two_new: float32 [1024, 512], P(('wide', 'narrow'))
The draws below stay inside these ranges and needn't reach their ends.
Inputs may be any that keep to these rules, and one draw needn't show every extreme that they name: `lengths`: some sequence has exactly 256 live positions. `item_rows`: A row r has inner block index (r // 32) % 4. In every sequence at most 128 of the 256 positions name rows of one inner block index, and some index is named by exactly 128 of them.
All inputs are finite; a program needn't handle non-finite values.
Results may differ from the reference program's by a relative error of at most 0.005.
Values may be sent and summed in bfloat16 or wider, within the bound.
No kernel may reach another device: no remote copies, remote signals or barrier semaphores. Data moves between devices by JAX's collectives and lax.ppermute only.
A program may use at most 64 MiB of HBM per device.

```python
import math
import jax
import jax.numpy as jnp
from jax import lax

D = 512
HEADS = 8
MICRO = 2
LMAX = 256
ROWS_DEV = 32
SEQS = 64
ITEMS = 1024
CAP = 128
N_WIDE = 8
N_NARROW = 4


def draw_lengths(key, part):
    first_key, second_key = jax.random.split(jax.random.fold_in(key, 11))
    heavy_low = jax.random.randint(first_key, (SEQS,), 13 * LMAX // 16, LMAX + 1)
    light_low = jax.random.randint(jax.random.fold_in(first_key, 5), (SEQS,), 5 * LMAX // 8, 13 * LMAX // 16)
    wide_index = jnp.arange(SEQS) // (MICRO * N_NARROW)
    values = jnp.where(wide_index < N_WIDE // 2, heavy_low, light_low)
    chosen = jax.random.randint(second_key, (), 0, SEQS)
    return jnp.where(jnp.arange(SEQS) == chosen, LMAX, values).astype(jnp.int32)


def draw_item_rows(key, part):
    base_key = jax.random.fold_in(key, 23)
    owned = N_WIDE * ROWS_DEV
    order_keys = jax.random.split(jax.random.fold_in(base_key, 1), N_NARROW)
    orders = jax.vmap(lambda order_key: jax.random.permutation(order_key, owned))(order_keys)
    sequence_keys = jax.random.split(jax.random.fold_in(base_key, 2), SEQS)

    def one_sequence(seq_key):
        key_full, key_other, key_place, key_left, key_right = jax.random.split(seq_key, 5)
        full_owner = jax.random.randint(key_full, (), 0, N_NARROW)
        others = jax.random.permutation(key_other, (N_NARROW - 1) * CAP)[:LMAX - CAP]
        other_owner = (full_owner + 1 + others // CAP) % N_NARROW
        owner_all = jnp.concatenate([jnp.full((CAP,), full_owner, jnp.int32), other_owner.astype(jnp.int32)])
        owner_seq = owner_all[jax.random.permutation(key_place, LMAX)]
        left_draw = jax.random.randint(key_left, (LMAX,), 0, owned)
        right_draw = jax.random.randint(key_right, (LMAX,), 0, owned)
        skewed = left_draw * right_draw // owned
        local_row = orders[owner_seq, skewed]
        outer_block = local_row // ROWS_DEV
        within = local_row % ROWS_DEV
        return ((outer_block * N_NARROW + owner_seq) * ROWS_DEV + within).astype(jnp.int32)
    return jax.vmap(one_sequence)(sequence_keys)


def block_levels(own_key, dims, cuts, low, high):
    factor_of, own = 1.0, jax.random.fold_in(own_key, 6)
    for dim, parts in cuts:
        draws = jnp.exp(jax.random.uniform(jax.random.fold_in(own, dim), (parts,), jnp.float32, low / len(cuts), high / len(cuts)))
        factor_of = factor_of * jnp.repeat(draws, dims[dim] // parts).reshape([-1 if axis == dim else 1 for axis in range(len(dims))])
    return factor_of


def scatter_about(key, shape, spread, most, cuts=(), dtype=jnp.bfloat16):
    level = block_levels(key, shape, cuts, -0.22, 0.18) if cuts else 1.0
    array = jax.random.normal(key, shape, jnp.float32) * spread * level
    return jnp.minimum(jnp.maximum(array, -most), most).astype(dtype)


def setup_inputs(seed: int = 0) -> dict:
    key_list = jax.random.split(jax.random.key(seed), 10)
    return {
        "tokens": scatter_about(key_list[0], (SEQS, LMAX, D), 1.0, 6.0, ((0, 32),)),
        "cotangent": scatter_about(key_list[1], (SEQS, LMAX, D), 0.05, 0.29882812, ((0, 32),)),
        "lengths": draw_lengths(jax.random.fold_in(key_list[9], 71), 0),
        "item_rows": draw_item_rows(jax.random.fold_in(key_list[9], 71), 0),
        "w_in": scatter_about(key_list[4], (D, 4 * D), D ** -0.5, 0.25),
        "w_out": scatter_about(key_list[5], (D, D), D ** -0.5, 0.25),
        "table": scatter_about(key_list[6], (ITEMS, D), 1.0, 6.0, ((0, 32),), jnp.float32),
        "moment_one": scatter_about(key_list[7], (ITEMS, D), 0.05, 0.3, ((0, 32),), jnp.float32),
        "moment_two": jnp.clip(jnp.exp(math.log(0.01) - 4.6051702 * jax.random.uniform(key_list[8], (ITEMS, D), jnp.float32) ** block_levels(key_list[8], (ITEMS, D), ((0, 32),), -0.2, 0.2)), 0.0001, 0.01),
    }


norm_eps = 1e-06
clip_norm = 4.0
learn_rate = 0.5
beta_first = 0.9
beta_second = 0.999
adam_step = 3.0
adam_eps = 1e-08

def layer_forward(source, w_in, w_out, length):
    positions, width = source.shape
    per_head = width // HEADS
    inner = jnp.dot(source.astype(jnp.bfloat16), w_in, preferred_element_type=jnp.float32)
    hidden = jax.nn.silu(inner).astype(jnp.bfloat16)
    gate_part, value_part, query_part, key_part = jnp.split(hidden, 4, axis=1)
    query_part = query_part.reshape(positions, HEADS, per_head).astype(jnp.float32)
    key_part = key_part.reshape(positions, HEADS, per_head).astype(jnp.float32)
    value_part = value_part.reshape(positions, HEADS, per_head).astype(jnp.float32)
    scores = jnp.einsum('qhd,khd->hqk', query_part, key_part) * per_head ** (-0.5)
    index_row = jnp.arange(positions)
    allowed = ((index_row[None, :] <= index_row[:, None]) & (index_row[:, None] < length)).astype(jnp.float32)
    attention = (jax.nn.silu(scores) * allowed[None] / length.astype(jnp.float32)).astype(jnp.bfloat16)
    mixed = jnp.einsum('hqk,khd->qhd', attention.astype(jnp.float32), value_part).reshape(positions, width)
    centered = mixed - lax.optimization_barrier(jnp.mean(mixed, axis=1, keepdims=True))
    normed = centered * lax.rsqrt(lax.optimization_barrier(jnp.mean(centered * centered, axis=1, keepdims=True)) + norm_eps)
    gated = (normed * gate_part.astype(jnp.float32)).astype(jnp.bfloat16)
    return jnp.dot(gated, w_out, preferred_element_type=jnp.float32) + source

def token_grads(inputs, cotangent, length, w_in, w_out):
    live_mask = (jnp.arange(inputs.shape[0]) < length).astype(jnp.float32)
    _, pullback = jax.vjp(lambda source_rows: layer_forward(source_rows, w_in, w_out, length), inputs.astype(jnp.float32))
    gradient, = pullback(cotangent.astype(jnp.float32) * live_mask[:, None])
    return gradient.astype(jnp.bfloat16)

def adam_rows(row_grad, table, moment_one, moment_two):
    row_norms = jnp.sqrt(lax.optimization_barrier(jnp.sum(row_grad * row_grad, axis=1, keepdims=True)))
    clipped = row_grad * (clip_norm / jnp.maximum(row_norms, clip_norm))
    first_moment = beta_first * moment_one + (1.0 - beta_first) * clipped
    second_moment = beta_second * moment_two + (1.0 - beta_second) * clipped * clipped
    step_size = learn_rate / (1.0 - beta_first ** adam_step)
    scaled = jnp.sqrt(second_moment / (1.0 - beta_second ** adam_step)) + adam_eps
    return (table - step_size * first_moment / scaled, first_moment, second_moment)

def reference(tokens, cotangent, lengths, item_rows, w_in, w_out, table, moment_one, moment_two):
    gradients = lax.map(lambda pieces: token_grads(pieces[0], pieces[1], pieces[2], w_in, w_out), (tokens, cotangent, lengths))
    flat_rows = gradients.reshape(-1, gradients.shape[-1]).astype(jnp.float32)
    row_grad = jax.ops.segment_sum(flat_rows, item_rows.reshape(-1).astype(jnp.int32), num_segments=ITEMS)
    return adam_rows(row_grad, table, moment_one, moment_two)
```

```python
import functools

import jax
import jax.numpy as jnp
from jax import lax
from jax.experimental import pallas as pl
from jax.experimental.pallas import tpu as pltpu
from jax.sharding import PartitionSpec as P

HEADS = 8
CORES = 2
LANES = 128

norm_eps = 1e-06
clip_norm = 4.0
learn_rate = 0.5
beta_first = 0.9
beta_second = 0.999
adam_step = 3.0
adam_eps = 1e-08

AXES = ("wide", "narrow")


def layout_of(wide, narrow):
    cores = CORES if narrow % CORES == 0 else 1
    inner = 2 if wide % 2 == 0 else 1
    return cores, inner, narrow // cores, wide // inner


def destination(wide, narrow, w, n, cr, ir, yr, zr):
    cores, inner, pairs, outer = layout_of(wide, narrow)
    z, i = w // inner, w % inner
    y, c = n // cores, n % cores
    w_to = ((z + zr) % outer) * inner + (i + ir) % inner
    n_to = ((y + yr) % pairs) * cores + (c + cr) % cores
    return w_to, n_to


def send(x, wide, narrow, offset):
    perm = []
    for w in range(wide):
        for n in range(narrow):
            w_to, n_to = destination(wide, narrow, w, n, *offset)
            perm.append((w * narrow + n, w_to * narrow + n_to))
    return lax.ppermute(x, AXES, perm)


def dot(a, b):
    return lax.dot_general(a, b, (((1,), (0,)), ((), ())), preferred_element_type=jnp.float32)


def dot_nt(a, b):
    return lax.dot_general(a, b, (((1,), (1,)), ((), ())), preferred_element_type=jnp.float32)


def sigmoid(x):
    return 1.0 / (1.0 + jnp.exp(-x))


def local_kernel(
    wide, narrow, rows_dev,
    len_ref, rows_ref, tok_ref, cot_ref, win_ref, wout_ref,
    part_ref,
    hid, slope, att, fac, mixed, inner_grad, dgated, grads, dm_t, q_t, dk_t, dv_t,
):
    micro, lmax, width = tok_ref.shape
    half = lmax // 2
    per_head = width // HEADS
    f32, bf16 = jnp.float32, jnp.bfloat16
    total = micro * lmax

    source = tok_ref[...].reshape(total, width)
    tile = 256
    for t in range(4 * width // tile):
        cols = pl.ds(t * tile, tile)
        inner = dot(source, win_ref[:, cols])
        gate_s = sigmoid(inner)
        act = inner * gate_s
        hid[:, cols] = act.astype(bf16)
        slope[:, cols] = gate_s + act * (1.0 - gate_s)

    row = lax.broadcasted_iota(jnp.int32, (lmax, 1), 0)
    for s in range(micro):
        live = (row < len_ref[s]).astype(f32)
        masked = (cot_ref[s].astype(f32) * live).astype(bf16)
        grads[pl.ds(s * lmax, lmax), :] = masked
    dgated[...] = dot_nt(grads[...], wout_ref[...]).astype(bf16)

    lane = lax.broadcasted_iota(jnp.int32, (1, LANES), 1)
    heads_here = LANES // per_head
    masks = [((lane // per_head) == h).astype(bf16) for h in range(heads_here)]
    scale = per_head ** (-0.5)
    causal = lax.broadcasted_iota(jnp.int32, (half, half), 1) <= lax.broadcasted_iota(jnp.int32, (half, half), 0)
    none = jnp.zeros((half, half), bf16)

    def one_sequence(s, carry):
        base = pl.multiple_of(s * lmax, lmax)
        here = pl.ds(base, lmax)
        length = len_ref[s]
        share = jnp.where(row < length, 1.0 / jnp.full((lmax, 1), length, jnp.int32).astype(f32), 0.0)

        for p in range(width // LANES):
            q = hid[here, pl.ds(2 * width + p * LANES, LANES)]
            k = hid[here, pl.ds(3 * width + p * LANES, LANES)]
            v = hid[here, pl.ds(width + p * LANES, LANES)]
            weights, values = [], []
            for h in range(heads_here):
                head = p * heads_here + h
                qm = q * (masks[h] * jnp.asarray(scale, bf16))
                parts = []
                for b in range(2):
                    rows = slice(b * half, (b + 1) * half)
                    score = dot_nt(qm[rows], k[: (b + 1) * half])
                    gate_s = sigmoid(score)
                    act = score * gate_s
                    part = share[rows]
                    if b == 0:
                        w_b = jnp.where(causal, act * part, 0.0)
                        f_b = jnp.where(causal, (gate_s + act * (1.0 - gate_s)) * (part * scale), 0.0)
                        fac[head, :half, :half] = f_b
                        parts.append(jnp.concatenate([w_b.astype(bf16), none], axis=1))
                    else:
                        w_b = act * part
                        f_b = (gate_s + act * (1.0 - gate_s)) * (part * scale)
                        fac[head, half:, :half] = f_b[:, :half]
                        fac[head, half:, half:] = jnp.where(causal, f_b[:, half:], 0.0)
                        parts.append(
                            jnp.concatenate(
                                [w_b[:, :half].astype(bf16), jnp.where(causal, w_b[:, half:], 0.0).astype(bf16)], axis=1
                            )
                        )
                weight = jnp.concatenate(parts, axis=0)
                att[head] = weight
                weights.append(weight)
                values.append(v * masks[h])
            mixed[:, pl.ds(p * LANES, LANES)] = dot(
                jnp.concatenate(weights, axis=1), jnp.concatenate(values, axis=0)
            )

        mix = mixed[...]
        centered = mix - jnp.mean(mix, axis=1, keepdims=True)
        inv = lax.rsqrt(jnp.mean(centered * centered, axis=1, keepdims=True) + norm_eps)
        normed = centered * inv
        dg = dgated[here, :].astype(f32)
        gate = hid[here, pl.ds(0, width)].astype(f32)
        dgate = (dg * normed).astype(bf16).astype(f32)
        inner_grad[here, pl.ds(0, width)] = (dgate * slope[here, pl.ds(0, width)]).astype(bf16)
        dn = dg * gate
        dmix = inv * (
            dn - jnp.mean(dn, axis=1, keepdims=True) - normed * jnp.mean(dn * normed, axis=1, keepdims=True)
        )
        dm = dmix.astype(bf16)
        dm_t[...] = dm.T
        q_t[...] = hid[here, pl.ds(2 * width, width)].T

        for p in range(width // LANES):
            k = hid[here, pl.ds(3 * width + p * LANES, LANES)]
            v = hid[here, pl.ds(width + p * LANES, LANES)]
            dmp = dm[:, p * LANES : (p + 1) * LANES]
            scores, keys = [], []
            for h in range(heads_here):
                head = p * heads_here + h
                dmm = dmp * masks[h]
                d_top = dot_nt(dmm[:half], v[:half]).astype(bf16).astype(f32)
                d_low = dot_nt(dmm[half:], v).astype(bf16).astype(f32)
                ds_top = (d_top * fac[head, :half, :half]).astype(bf16)
                ds_low = (d_low * fac[head, half:, :]).astype(bf16)
                ds = jnp.concatenate([jnp.concatenate([ds_top, none], axis=1), ds_low], axis=0)
                scores.append(ds)
                keys.append(k * masks[h])
                feat = pl.ds(head * per_head, per_head)
                dk_t[feat, :] = dot(q_t[feat, :], ds).astype(bf16)
                dv_t[feat, :] = dot(dm_t[feat, :], att[head]).astype(bf16)
            dq = dot(jnp.concatenate(scores, axis=1), jnp.concatenate(keys, axis=0)).astype(bf16).astype(f32)
            cols = pl.ds(2 * width + p * LANES, LANES)
            inner_grad[here, cols] = (dq * slope[here, cols]).astype(bf16)
        for part, source_t in ((1, dv_t), (3, dk_t)):
            cols = pl.ds(part * width, width)
            inner_grad[here, cols] = (source_t[...].T.astype(f32) * slope[here, cols]).astype(bf16)
        return carry

    lax.fori_loop(0, micro, one_sequence, 0)

    back = dot_nt(inner_grad[...], win_ref[...]).astype(bf16).astype(f32)
    grads[...] = (back + grads[...].astype(f32)).astype(bf16)

    cores, inner_w, pairs, outer = layout_of(wide, narrow)
    w_me, n_me = lax.axis_index("wide"), lax.axis_index("narrow")
    z_me, i_me = w_me // inner_w, w_me % inner_w
    y_me, c_me = n_me // cores, n_me % cores
    per_chunk = 8
    slot = lax.broadcasted_iota(jnp.int32, (rows_dev, lmax), 0)

    def one_chunk(j, carry):
        pieces = []
        for b in range(per_chunk):
            block = j * per_chunk + b
            zr = block % outer
            yr = (block // outer) % pairs
            ir = (block // (outer * pairs)) % inner_w
            cr = block // (outer * pairs * inner_w)
            w_to = ((z_me + zr) % outer) * inner_w + (i_me + ir) % inner_w
            n_to = ((y_me + yr) % pairs) * cores + (c_me + cr) % cores
            first = (w_to * narrow + n_to) * rows_dev
            want = slot + first
            pieces.append(
                jnp.concatenate(
                    [(want == rows_ref[s : s + 1, :]).astype(f32).astype(bf16) for s in range(micro)], axis=1
                )
            )
        chosen = jnp.concatenate(pieces, axis=0)
        size = per_chunk * rows_dev
        part_ref[pl.ds(pl.multiple_of(j * size, size), size), :] = dot(chosen, grads[...]).astype(bf16)
        return carry

    chunks = wide * narrow // per_chunk
    lax.fori_loop(0, chunks, one_chunk, 0)


def local_rows(wide, narrow, rows_dev, tokens, cotangent, lengths, item_rows, w_in, w_out):
    micro, lmax, width = tokens.shape
    total = micro * lmax
    items = wide * narrow * rows_dev
    f32, bf16 = jnp.float32, jnp.bfloat16
    vmem = pl.BlockSpec(memory_space=pltpu.VMEM)
    return pl.pallas_call(
        functools.partial(local_kernel, wide, narrow, rows_dev),
        out_shape=jax.ShapeDtypeStruct((items, width), bf16),
        in_specs=[pl.BlockSpec(memory_space=pltpu.SMEM)] + [vmem] * 5,
        out_specs=vmem,
        scratch_shapes=[
            pltpu.VMEM((total, 4 * width), bf16),
            pltpu.VMEM((total, 4 * width), f32),
            pltpu.VMEM((HEADS, lmax, lmax), bf16),
            pltpu.VMEM((HEADS, lmax, lmax), f32),
            pltpu.VMEM((lmax, width), f32),
            pltpu.VMEM((total, 4 * width), bf16),
            pltpu.VMEM((total, width), bf16),
            pltpu.VMEM((total, width), bf16),
            pltpu.VMEM((width, lmax), bf16),
            pltpu.VMEM((width, lmax), bf16),
            pltpu.VMEM((width, lmax), bf16),
            pltpu.VMEM((width, lmax), bf16),
        ],
        cost_estimate=pl.CostEstimate(
            flops=16 * total * width * width + 12 * total * lmax * width,
            bytes_accessed=4 * total * width + 10 * width * width + 2 * items * width,
            transcendentals=HEADS * total * lmax,
        ),
        name="local_rows",
    )(lengths, item_rows, tokens, cotangent, w_in, w_out)


def adam_rows(row_grad, table, moment_one, moment_two):
    row_norms = jnp.sqrt(jnp.sum(row_grad * row_grad, axis=1, keepdims=True))
    clipped = row_grad * (clip_norm / jnp.maximum(row_norms, clip_norm))
    first_moment = beta_first * moment_one + (1.0 - beta_first) * clipped
    second_moment = beta_second * moment_two + (1.0 - beta_second) * clipped * clipped
    step_size = learn_rate / (1.0 - beta_first**adam_step)
    scaled = jnp.sqrt(second_moment / (1.0 - beta_second**adam_step)) + adam_eps
    return (table - step_size * first_moment / scaled, first_moment, second_moment)


def gather_sum(x, offsets, wide, narrow):
    arrived = [send(x[k], wide, narrow, offsets[k]) for k in range(1, len(offsets))]
    out = x[0].astype(jnp.float32)
    for piece in arrived:
        out = out + piece.astype(jnp.float32)
    return out


def on_device(tokens, cotangent, lengths, item_rows, w_in, w_out, table, moment_one, moment_two):
    wide, narrow = lax.axis_size("wide"), lax.axis_size("narrow")
    rows_dev, width = table.shape
    cores, inner, pairs, outer = layout_of(wide, narrow)
    partial = local_rows(wide, narrow, rows_dev, tokens, cotangent, lengths, item_rows, w_in, w_out)
    stages = (
        [(c, 0, 0, 0) for c in range(cores)],
        [(0, i, y, 0) for i in range(inner) for y in range(pairs)],
        [(0, 0, 0, z) for z in range(outer)],
    )
    held = partial
    for offsets in stages:
        held = held.astype(jnp.bfloat16).reshape(len(offsets), -1, width)
        held = gather_sum(held, offsets, wide, narrow)
    return adam_rows(held, table, moment_one, moment_two)


def solution(mesh):
    return jax.shard_map(
        on_device,
        mesh=mesh,
        in_specs=(
            P(AXES, None, None),
            P(AXES, None, None),
            P(AXES),
            P(AXES, None),
            P(),
            P(),
            P(AXES, None),
            P(AXES, None),
            P(AXES, None),
        ),
        out_specs=(P(AXES, None), P(AXES, None), P(AXES, None)),
        check_vma=False,
    )
```

```python
import functools

import jax
import jax.numpy as jnp
from jax import lax
from jax.experimental import pallas as pl
from jax.experimental.pallas import tpu as pltpu
from jax.sharding import PartitionSpec as P

HEADS = 8
CORES = 2
LANES = 128

norm_eps = 1e-06
clip_norm = 4.0
learn_rate = 0.5
beta_first = 0.9
beta_second = 0.999
adam_step = 3.0
adam_eps = 1e-08

AXES = ("wide", "narrow")


def layout_of(wide, narrow):
    cores = CORES
    inner = 2 if wide % 2 == 0 else 1
    return cores, inner, narrow // cores, wide // inner


def destination(wide, narrow, w, n, cr, ir, yr, zr):
    cores, inner, pairs, outer = layout_of(wide, narrow)
    z, i = w // inner, w % inner
    y, c = n // cores, n % cores
    w_to = ((z + zr) % outer) * inner + (i + ir) % inner
    n_to = ((y + yr) % pairs) * cores + (c + cr) % cores
    return w_to, n_to


def send(x, wide, narrow, offset):
    perm = []
    for w in range(wide):
        for n in range(narrow):
            w_to, n_to = destination(wide, narrow, w, n, *offset)
            perm.append((w * narrow + n, w_to * narrow + n_to))
    return lax.ppermute(x, AXES, perm)


def dot(a, b):
    return lax.dot_general(a, b, (((1,), (0,)), ((), ())), preferred_element_type=jnp.float32)


def dot_nt(a, b):
    return lax.dot_general(a, b, (((1,), (1,)), ((), ())), preferred_element_type=jnp.float32)


def local_kernel(
    wide, narrow, rows_dev,
    len_hbm, rows_hbm, tok_hbm, cot_hbm, win_hbm, wout_hbm,
    keep_ref, send_ref,
    len_ref, rows_ref, tok, cot, win, wout, hid, slope, att, fac, mixed, inner_grad, dgated, dm_s, dm_t, q_t, dk_t, dv_t, sems,
):
    micro, lmax, width = tok_hbm.shape
    half = lmax // 2
    per_head = width // HEADS
    f32, bf16 = jnp.float32, jnp.bfloat16
    total = micro * lmax
    tile = 256
    tiles = 4 * width // tile

    copies = [pltpu.make_async_copy(tok_hbm, tok, sems.at[0])]
    for t in range(tiles):
        cols = pl.ds(t * tile, tile)
        copies.append(pltpu.make_async_copy(win_hbm.at[:, cols], win.at[:, cols], sems.at[1 + t]))
    copies.append(pltpu.make_async_copy(cot_hbm, cot, sems.at[1 + tiles]))
    copies.append(pltpu.make_async_copy(wout_hbm, wout, sems.at[2 + tiles]))
    copies.append(pltpu.make_async_copy(len_hbm, len_ref, sems.at[3 + tiles]))
    copies.append(pltpu.make_async_copy(rows_hbm, rows_ref, sems.at[4 + tiles]))
    for copy in copies:
        copy.start()

    copies[0].wait()
    source = tok[...].reshape(total, width) * jnp.asarray(0.5, bf16)
    for t in range(tiles):
        cols = pl.ds(t * tile, tile)
        copies[1 + t].wait()
        u = dot(source, win[:, cols])
        th = jnp.tanh(u)
        up = 1.0 + th
        act = u * up
        hid[:, cols] = act.astype(bf16)
        slope[:, cols] = up + act * (1.0 - th)

    row = lax.broadcasted_iota(jnp.int32, (lmax, 1), 0)
    copies[1 + tiles].wait()
    copies[3 + tiles].wait()
    for s in range(micro):
        live = (row < len_ref[s]).astype(f32)
        cot[s] = (cot[s].astype(f32) * live).astype(bf16)
    copies[2 + tiles].wait()
    dgated[...] = dot_nt(cot[...].reshape(total, width), wout[...]).astype(bf16)

    lane = lax.broadcasted_iota(jnp.int32, (1, LANES), 1)
    heads_here = LANES // per_head
    masks = [((lane // per_head) == h).astype(bf16) for h in range(heads_here)]
    scale = per_head ** (-0.5)
    causal = lax.broadcasted_iota(jnp.int32, (half, half), 1) <= lax.broadcasted_iota(jnp.int32, (half, half), 0)
    none = jnp.zeros((half, half), bf16)

    def pick_lanes(stacked):
        out = stacked[:lmax]
        for h in range(1, heads_here):
            out = jnp.where(lane // per_head == h, stacked[h * lmax : (h + 1) * lmax], out)
        return out

    def one_sequence(s, carry):
        base = pl.multiple_of(s * lmax, lmax)
        here = pl.ds(base, lmax)
        length = len_ref[s]
        share = jnp.where(row < length, 1.0 / jnp.full((lmax, 1), length, jnp.int32).astype(f32), 0.0)
        share_half = share * (0.5 * scale)

        for p in range(width // LANES):
            q = hid[here, pl.ds(2 * width + p * LANES, LANES)]
            k = hid[here, pl.ds(3 * width + p * LANES, LANES)]
            v = hid[here, pl.ds(width + p * LANES, LANES)]
            qs = jnp.concatenate([q * (m * jnp.asarray(0.5 * scale, bf16)) for m in masks], axis=0)
            scores = dot_nt(qs, k)
            weights = []
            for h in range(heads_here):
                head = p * heads_here + h
                parts = []
                for b in range(2):
                    rows = slice(b * half, (b + 1) * half)
                    u = scores[h * lmax + b * half : h * lmax + (b + 1) * half, : (b + 1) * half]
                    th = jnp.tanh(u)
                    up = 1.0 + th
                    act = u * up
                    w_b = act * share[rows]
                    f_b = (up + act * (1.0 - th)) * share_half[rows]
                    edge = slice(b * half, (b + 1) * half)
                    diag = jnp.where(causal, w_b[:, edge], 0.0).astype(bf16)
                    fac[head, rows, edge] = jnp.where(causal, f_b[:, edge], 0.0)
                    if b == 0:
                        parts.append(jnp.concatenate([diag, none], axis=1))
                    else:
                        fac[head, rows, :half] = f_b[:, :half]
                        parts.append(jnp.concatenate([w_b[:, :half].astype(bf16), diag], axis=1))
                weight = jnp.concatenate(parts, axis=0)
                att[head] = weight
                weights.append(weight)
            mixed[:, pl.ds(p * LANES, LANES)] = pick_lanes(dot(jnp.concatenate(weights, axis=0), v))

        group = 32
        for r in range(lmax // group):
            rows = pl.ds(r * group, group)
            those = pl.ds(pl.multiple_of(base + r * group, group), group)
            mix = mixed[rows, :]
            centered = mix - jnp.mean(mix, axis=1, keepdims=True)
            inv = lax.rsqrt(jnp.mean(centered * centered, axis=1, keepdims=True) + norm_eps)
            normed = centered * inv
            dg = dgated[those, :].astype(f32)
            gate = hid[those, pl.ds(0, width)].astype(f32)
            dgate = (dg * normed).astype(bf16).astype(f32)
            inner_grad[those, pl.ds(0, width)] = (dgate * slope[those, pl.ds(0, width)]).astype(bf16)
            dn = dg * gate
            dmix = inv * (
                dn - jnp.mean(dn, axis=1, keepdims=True) - normed * jnp.mean(dn * normed, axis=1, keepdims=True)
            )
            dm_s[rows, :] = dmix.astype(bf16)
        dm_t[...] = dm_s[...].T
        q_t[...] = hid[here, pl.ds(2 * width, width)].T

        for p in range(width // LANES):
            k = hid[here, pl.ds(3 * width + p * LANES, LANES)]
            v = hid[here, pl.ds(width + p * LANES, LANES)]
            dmp = dm_s[:, pl.ds(p * LANES, LANES)]
            d_att = dot_nt(jnp.concatenate([dmp * m for m in masks], axis=0), v)
            stacked = []
            for h in range(heads_here):
                head = p * heads_here + h
                d_top = d_att[h * lmax : h * lmax + half, :half].astype(bf16).astype(f32)
                d_low = d_att[h * lmax + half : (h + 1) * lmax].astype(bf16).astype(f32)
                ds_top = (d_top * fac[head, :half, :half]).astype(bf16)
                ds_low = (d_low * fac[head, half:, :]).astype(bf16)
                ds = jnp.concatenate([jnp.concatenate([ds_top, none], axis=1), ds_low], axis=0)
                stacked.append(ds)
                feat = pl.ds(head * per_head, per_head)
                dk_t[feat, :] = dot(q_t[feat, :], ds).astype(bf16)
                dv_t[feat, :] = dot(dm_t[feat, :], att[head]).astype(bf16)
            dq = pick_lanes(dot(jnp.concatenate(stacked, axis=0), k)).astype(bf16).astype(f32)
            cols = pl.ds(2 * width + p * LANES, LANES)
            inner_grad[here, cols] = (dq * slope[here, cols]).astype(bf16)
        for part, source_t in ((1, dv_t), (3, dk_t)):
            cols = pl.ds(part * width, width)
            inner_grad[here, cols] = (source_t[...].T.astype(f32) * slope[here, cols]).astype(bf16)
        return carry

    lax.fori_loop(0, micro, one_sequence, 0)

    back = (0.5 * dot_nt(inner_grad[...], win[...])).astype(bf16).astype(f32)
    grads = (back + cot[...].reshape(total, width).astype(f32)).astype(bf16)
    dgated[...] = grads

    copies[4 + tiles].wait()
    cores, inner_w, pairs, outer = layout_of(wide, narrow)
    w_me, n_me = lax.axis_index("wide"), lax.axis_index("narrow")
    z_me, i_me = w_me // inner_w, w_me % inner_w
    y_me, c_me = n_me // cores, n_me % cores
    blocks = wide * narrow // cores
    per_chunk = min(8, blocks)
    size = per_chunk * rows_dev
    slot = lax.broadcasted_iota(jnp.int32, (rows_dev, lmax), 0)

    def fill(out_ref, core_offset):
        def one_chunk(j, carry):
            pieces = []
            for b in range(per_chunk):
                block = j * per_chunk + b
                zr = block % outer
                yr = (block // outer) % pairs
                ir = block // (outer * pairs)
                w_to = ((z_me + zr) % outer) * inner_w + (i_me + ir) % inner_w
                n_to = ((y_me + yr) % pairs) * cores + (c_me + core_offset) % cores
                want = slot + (w_to * narrow + n_to) * rows_dev
                pieces.append(
                    jnp.concatenate(
                        [(want == rows_ref[s : s + 1, :]).astype(f32).astype(bf16) for s in range(micro)], axis=1
                    )
                )
            chosen = jnp.concatenate(pieces, axis=0)
            out_ref[pl.ds(pl.multiple_of(j * size, size), size), :] = dot(chosen, dgated[...]).astype(bf16)
            return carry

        lax.fori_loop(0, blocks // per_chunk, one_chunk, 0, unroll=blocks // per_chunk <= 4)

    fill(send_ref, 1)
    fill(keep_ref, 0)


def local_rows(wide, narrow, rows_dev, tokens, cotangent, lengths, item_rows, w_in, w_out):
    micro, lmax, width = tokens.shape
    total = micro * lmax
    items = wide * narrow * rows_dev
    f32, bf16 = jnp.float32, jnp.bfloat16
    vmem = pl.BlockSpec(memory_space=pltpu.VMEM)
    hbm = pl.BlockSpec(memory_space=pltpu.HBM)
    part = jax.ShapeDtypeStruct((items // CORES, width), bf16)
    tiles = 4 * width // 256
    return pl.pallas_call(
        functools.partial(local_kernel, wide, narrow, rows_dev),
        out_shape=(part, part),
        in_specs=[hbm] * 6,
        out_specs=(vmem, vmem),
        scratch_shapes=[
            pltpu.SMEM((micro,), jnp.int32),
            pltpu.VMEM((micro, lmax), jnp.int32),
            pltpu.VMEM((micro, lmax, width), bf16),
            pltpu.VMEM((micro, lmax, width), bf16),
            pltpu.VMEM((width, 4 * width), bf16),
            pltpu.VMEM((width, width), bf16),
            pltpu.VMEM((total, 4 * width), bf16),
            pltpu.VMEM((total, 4 * width), f32),
            pltpu.VMEM((HEADS, lmax, lmax), bf16),
            pltpu.VMEM((HEADS, lmax, lmax), f32),
            pltpu.VMEM((lmax, width), f32),
            pltpu.VMEM((total, 4 * width), bf16),
            pltpu.VMEM((total, width), bf16),
            pltpu.VMEM((lmax, width), bf16),
            pltpu.VMEM((width, lmax), bf16),
            pltpu.VMEM((width, lmax), bf16),
            pltpu.VMEM((width, lmax), bf16),
            pltpu.VMEM((width, lmax), bf16),
            pltpu.SemaphoreType.DMA((tiles + 5,)),
        ],
        compiler_params=pltpu.CompilerParams(vmem_limit_bytes=(28 << 20) + 4 * items * width),
        cost_estimate=pl.CostEstimate(
            flops=16 * total * width * width + 12 * total * lmax * width,
            bytes_accessed=4 * total * width + 10 * width * width + 2 * items * width,
            transcendentals=HEADS * total * lmax,
        ),
        name="local_rows",
    )(*(pltpu.with_memory_space_constraint(a, pltpu.HBM) for a in (lengths, item_rows, tokens, cotangent, w_in, w_out)))


def adam_rows(row_grad, table, moment_one, moment_two):
    row_norms = jnp.sqrt(jnp.sum(row_grad * row_grad, axis=1, keepdims=True))
    clipped = row_grad * (clip_norm / jnp.maximum(row_norms, clip_norm))
    first_moment = beta_first * moment_one + (1.0 - beta_first) * clipped
    second_moment = beta_second * moment_two + (1.0 - beta_second) * clipped * clipped
    step_size = learn_rate / (1.0 - beta_first**adam_step)
    scaled = jnp.sqrt(second_moment / (1.0 - beta_second**adam_step)) + adam_eps
    return (table - step_size * first_moment / scaled, first_moment, second_moment)


def gather_sum(pieces, offsets, wide, narrow):
    arrived = [send(pieces[k], wide, narrow, offsets[k]) for k in range(1, len(offsets))]
    out = pieces[0].astype(jnp.float32)
    for piece in arrived:
        out = out + piece.astype(jnp.float32)
    return out


def on_device(tokens, cotangent, lengths, item_rows, w_in, w_out, table, moment_one, moment_two):
    wide, narrow = lax.axis_size("wide"), lax.axis_size("narrow")
    rows_dev, width = table.shape
    cores, inner, pairs, outer = layout_of(wide, narrow)
    held = local_rows(wide, narrow, rows_dev, tokens, cotangent, lengths, item_rows, w_in, w_out)
    stages = (
        [(c, 0, 0, 0) for c in range(cores)],
        [(0, i, y, 0) for i in range(inner) for y in range(pairs)],
        [(0, 0, 0, z) for z in range(outer)],
    )
    for number, offsets in enumerate(stages):
        if number:
            held = held.astype(jnp.bfloat16).reshape(len(offsets), -1, width)
        held = gather_sum(held, offsets, wide, narrow)
    return adam_rows(held, table, moment_one, moment_two)


def solution(mesh):
    return jax.shard_map(
        on_device,
        mesh=mesh,
        in_specs=(
            P(AXES, None, None),
            P(AXES, None, None),
            P(AXES),
            P(AXES, None),
            P(),
            P(),
            P(AXES, None),
            P(AXES, None),
            P(AXES, None),
        ),
        out_specs=(P(AXES, None), P(AXES, None), P(AXES, None)),
        check_vma=False,
    )
```

```python
import functools

import jax
import jax.numpy as jnp
from jax import lax
from jax.experimental import pallas as pl
from jax.experimental.pallas import tpu as pltpu
from jax.sharding import PartitionSpec as P

HEADS = 8
CORES = 2
LANES = 128

norm_eps = 1e-06
clip_norm = 4.0
learn_rate = 0.5
beta_first = 0.9
beta_second = 0.999
adam_step = 3.0
adam_eps = 1e-08

AXES = ("wide", "narrow")


def layout_of(wide, narrow):
    cores = CORES
    inner = 2 if wide % 2 == 0 else 1
    return cores, inner, narrow // cores, wide // inner


def destination(wide, narrow, w, n, cr, ir, yr, zr):
    cores, inner, pairs, outer = layout_of(wide, narrow)
    z, i = w // inner, w % inner
    y, c = n // cores, n % cores
    w_to = ((z + zr) % outer) * inner + (i + ir) % inner
    n_to = ((y + yr) % pairs) * cores + (c + cr) % cores
    return w_to, n_to


def send(x, wide, narrow, offset):
    perm = []
    for w in range(wide):
        for n in range(narrow):
            w_to, n_to = destination(wide, narrow, w, n, *offset)
            perm.append((w * narrow + n, w_to * narrow + n_to))
    return lax.ppermute(x, AXES, perm)


def dot(a, b):
    return lax.dot_general(a, b, (((1,), (0,)), ((), ())), preferred_element_type=jnp.float32)


def dot_nt(a, b):
    return lax.dot_general(a, b, (((1,), (1,)), ((), ())), preferred_element_type=jnp.float32)


def local_kernel(
    wide, narrow, rows_dev,
    len_hbm, rows_hbm, tok_hbm, cot_hbm, win_hbm, wout_hbm,
    keep_ref, send_ref,
    len_ref, rows_ref, tok, cot, win, wout, hid, slope, att, fac, mixed, inner_grad, dgated, dm_s, sems,
):
    micro, lmax, width = tok_hbm.shape
    half = lmax // 2
    per_head = width // HEADS
    f32, bf16 = jnp.float32, jnp.bfloat16
    total = micro * lmax
    bounds = (0, width, 2 * width, 4 * width)
    moves = [(tok_hbm, tok)]
    moves += [(win_hbm.at[:, lo:hi], win.at[:, lo:hi]) for lo, hi in zip(bounds, bounds[1:])]
    moves += [(wout_hbm, wout), (cot_hbm, cot), (len_hbm, len_ref), (rows_hbm, rows_ref)]
    copies = [pltpu.make_async_copy(src, dst, sems.at[i]) for i, (src, dst) in enumerate(moves)]
    for copy in copies:
        copy.start()

    tile = 256
    row = lax.broadcasted_iota(jnp.int32, (lmax, 1), 0)
    copies[0].wait()
    source = tok[...].reshape(total, width) * jnp.asarray(0.5, bf16)
    for part, (lo, hi) in enumerate(zip(bounds, bounds[1:])):
        copies[1 + part].wait()
        if hi == 4 * width:
            for copy in copies[len(bounds) :]:
                copy.wait()
            for s in range(micro):
                live = (row < len_ref[s]).astype(f32)
                cot[s] = (cot[s].astype(f32) * live).astype(bf16)
        for first in range(lo, hi, tile):
            cols = pl.ds(first, tile)
            u = dot(source, win[:, cols])
            th = jnp.tanh(u)
            up = 1.0 + th
            act = u * up
            hid[:, cols] = act.astype(bf16)
            slope[:, cols] = up + act * (1.0 - th)
    dgated[...] = dot_nt(cot[...].reshape(total, width), wout[...]).astype(bf16)

    lane = lax.broadcasted_iota(jnp.int32, (1, LANES), 1)
    heads_here = LANES // per_head
    masks = [((lane // per_head) == h).astype(bf16) for h in range(heads_here)]
    scale = per_head ** (-0.5)
    causal = lax.broadcasted_iota(jnp.int32, (half, half), 1) <= lax.broadcasted_iota(jnp.int32, (half, half), 0)
    none = jnp.zeros((half, half), bf16)
    lane_pairs = width // LANES
    group = 32
    groups = lmax // group

    def pick_lanes(stacked):
        out = stacked[:lmax]
        for h in range(1, heads_here):
            out = jnp.where(lane // per_head == h, stacked[h * lmax : (h + 1) * lmax], out)
        return out

    def forward_pair(s, p):
        here = pl.ds(s * lmax, lmax)
        length = len_ref[s]
        share = jnp.where(row < length, 1.0 / jnp.full((lmax, 1), length, jnp.int32).astype(f32), 0.0)
        share_half = share * (0.5 * scale)
        q = hid[here, pl.ds(2 * width + p * LANES, LANES)]
        k = hid[here, pl.ds(3 * width + p * LANES, LANES)]
        v = hid[here, pl.ds(width + p * LANES, LANES)]
        qs = jnp.concatenate([q * (m * jnp.asarray(0.5 * scale, bf16)) for m in masks], axis=0)
        scores = dot_nt(qs, k)
        weights = []
        for h in range(heads_here):
            head = p * heads_here + h
            parts = []
            for b in range(2):
                rows = slice(b * half, (b + 1) * half)
                u = scores[h * lmax + b * half : h * lmax + (b + 1) * half, : (b + 1) * half]
                th = jnp.tanh(u)
                up = 1.0 + th
                act = u * up
                w_b = act * share[rows]
                f_b = (up + act * (1.0 - th)) * share_half[rows]
                diag = jnp.where(causal, w_b[:, rows], 0.0).astype(bf16)
                fac[s, head, rows, rows] = jnp.where(causal, f_b[:, rows], 0.0)
                if b == 0:
                    parts.append(jnp.concatenate([diag, none], axis=1))
                else:
                    fac[s, head, rows, :half] = f_b[:, :half]
                    parts.append(jnp.concatenate([w_b[:, :half].astype(bf16), diag], axis=1))
            weight = jnp.concatenate(parts, axis=0)
            att[s, head] = weight
            weights.append(weight)
        mixed[s, :, pl.ds(p * LANES, LANES)] = pick_lanes(dot(jnp.concatenate(weights, axis=0), v))

    def norm_group(s, r):
        rows = pl.ds(r * group, group)
        those = pl.ds(s * lmax + r * group, group)
        mix = mixed[s, rows, :]
        centered = mix - jnp.mean(mix, axis=1, keepdims=True)
        inv = lax.rsqrt(jnp.mean(centered * centered, axis=1, keepdims=True) + norm_eps)
        normed = centered * inv
        dg = dgated[those, :].astype(f32)
        gate = hid[those, pl.ds(0, width)].astype(f32)
        dgate = (dg * normed).astype(bf16).astype(f32)
        inner_grad[those, pl.ds(0, width)] = (dgate * slope[those, pl.ds(0, width)]).astype(bf16)
        dn = dg * gate
        dmix = inv * (
            dn - jnp.mean(dn, axis=1, keepdims=True) - normed * jnp.mean(dn * normed, axis=1, keepdims=True)
        )
        dm_s[s, rows, :] = dmix.astype(bf16)

    def backward_pair(s, p):
        here = pl.ds(s * lmax, lmax)
        lanes = pl.ds(p * LANES, LANES)
        q_t = hid[here, pl.ds(2 * width + p * LANES, LANES)].T
        k = hid[here, pl.ds(3 * width + p * LANES, LANES)]
        v = hid[here, pl.ds(width + p * LANES, LANES)]
        dmp = dm_s[s, :, lanes]
        dm_t = dmp.T
        d_att = dot_nt(jnp.concatenate([dmp * m for m in masks], axis=0), v)
        stacked, dks, dvs = [], [], []
        for h in range(heads_here):
            head = p * heads_here + h
            feat = slice(h * per_head, (h + 1) * per_head)
            dvs.append(dot(dm_t[feat], att[s, head]).astype(bf16))
            d_top = d_att[h * lmax : h * lmax + half, :half].astype(bf16).astype(f32)
            d_low = d_att[h * lmax + half : (h + 1) * lmax].astype(bf16).astype(f32)
            ds_top = (d_top * fac[s, head, :half, :half]).astype(bf16)
            ds_low = (d_low * fac[s, head, half:, :]).astype(bf16)
            ds = jnp.concatenate([jnp.concatenate([ds_top, none], axis=1), ds_low], axis=0)
            stacked.append(ds)
            dks.append(dot(q_t[feat], ds).astype(bf16))
        dv = jnp.concatenate(dvs, axis=0).T.astype(f32)
        dk = jnp.concatenate(dks, axis=0).T.astype(f32)
        dq = pick_lanes(dot(jnp.concatenate(stacked, axis=0), k)).astype(bf16).astype(f32)
        for part, piece in ((1, dv), (2, dq), (3, dk)):
            cols = pl.ds(part * width + p * LANES, LANES)
            inner_grad[here, cols] = (piece * slope[here, cols]).astype(bf16)

    each = -(-groups // lane_pairs)
    norm_chunks = [range(p * each, min((p + 1) * each, groups)) for p in range(lane_pairs)]
    for s in range(micro):
        for p in range(lane_pairs):
            forward_pair(s, p)
            if s > 0:
                for r in norm_chunks[p]:
                    norm_group(s - 1, r)
        if s > 0:
            for p in range(lane_pairs):
                backward_pair(s - 1, p)
                if s == micro - 1:
                    for r in norm_chunks[p]:
                        norm_group(s, r)
    if micro == 1:
        for r in range(groups):
            norm_group(0, r)
    for p in range(lane_pairs):
        backward_pair(micro - 1, p)

    back = (0.5 * dot_nt(inner_grad[...], win[...])).astype(bf16).astype(f32)
    grads = (back + cot[...].reshape(total, width).astype(f32)).astype(bf16)
    dgated[...] = grads

    cores, inner_w, pairs, outer = layout_of(wide, narrow)
    w_me, n_me = lax.axis_index("wide"), lax.axis_index("narrow")
    z_me, i_me = w_me // inner_w, w_me % inner_w
    y_me, c_me = n_me // cores, n_me % cores
    blocks = wide * narrow // cores
    per_chunk = min(8, blocks)
    size = per_chunk * rows_dev
    slot = lax.broadcasted_iota(jnp.int32, (rows_dev, lmax), 0)

    def fill(out_ref, core_offset):
        def one_chunk(j, carry):
            pieces = []
            for b in range(per_chunk):
                block = j * per_chunk + b
                zr = block % outer
                yr = (block // outer) % pairs
                ir = block // (outer * pairs)
                w_to = ((z_me + zr) % outer) * inner_w + (i_me + ir) % inner_w
                n_to = ((y_me + yr) % pairs) * cores + (c_me + core_offset) % cores
                want = slot + (w_to * narrow + n_to) * rows_dev
                pieces.append(
                    jnp.concatenate(
                        [(want == rows_ref[s : s + 1, :]).astype(f32).astype(bf16) for s in range(micro)], axis=1
                    )
                )
            chosen = jnp.concatenate(pieces, axis=0)
            out_ref[pl.ds(pl.multiple_of(j * size, size), size), :] = dot(chosen, dgated[...]).astype(bf16)
            return carry

        lax.fori_loop(0, blocks // per_chunk, one_chunk, 0, unroll=blocks // per_chunk <= 4)

    fill(send_ref, 1)
    fill(keep_ref, 0)


def local_rows(wide, narrow, rows_dev, tokens, cotangent, lengths, item_rows, w_in, w_out):
    micro, lmax, width = tokens.shape
    total = micro * lmax
    items = wide * narrow * rows_dev
    f32, bf16 = jnp.float32, jnp.bfloat16
    vmem = pl.BlockSpec(memory_space=pltpu.VMEM)
    hbm = pl.BlockSpec(memory_space=pltpu.HBM)
    part = jax.ShapeDtypeStruct((items // CORES, width), bf16)
    return pl.pallas_call(
        functools.partial(local_kernel, wide, narrow, rows_dev),
        out_shape=(part, part),
        in_specs=[hbm] * 6,
        out_specs=(vmem, vmem),
        scratch_shapes=[
            pltpu.SMEM((micro,), jnp.int32),
            pltpu.VMEM((micro, lmax), jnp.int32),
            pltpu.VMEM((micro, lmax, width), bf16),
            pltpu.VMEM((micro, lmax, width), bf16),
            pltpu.VMEM((width, 4 * width), bf16),
            pltpu.VMEM((width, width), bf16),
            pltpu.VMEM((total, 4 * width), bf16),
            pltpu.VMEM((total, 4 * width), f32),
            pltpu.VMEM((micro, HEADS, lmax, lmax), bf16),
            pltpu.VMEM((micro, HEADS, lmax, lmax), f32),
            pltpu.VMEM((micro, lmax, width), f32),
            pltpu.VMEM((total, 4 * width), bf16),
            pltpu.VMEM((total, width), bf16),
            pltpu.VMEM((micro, lmax, width), bf16),
            pltpu.SemaphoreType.DMA((8,)),
        ],
        compiler_params=pltpu.CompilerParams(vmem_limit_bytes=(28 << 20) + 4 * items * width),
        cost_estimate=pl.CostEstimate(
            flops=16 * total * width * width + 12 * total * lmax * width,
            bytes_accessed=4 * total * width + 10 * width * width + 2 * items * width,
            transcendentals=HEADS * total * lmax,
        ),
        name="local_rows",
    )(*(pltpu.with_memory_space_constraint(a, pltpu.HBM) for a in (lengths, item_rows, tokens, cotangent, w_in, w_out)))


def adam_rows(row_grad, table, moment_one, moment_two):
    row_norms = jnp.sqrt(jnp.sum(row_grad * row_grad, axis=1, keepdims=True))
    clipped = row_grad * (clip_norm / jnp.maximum(row_norms, clip_norm))
    first_moment = beta_first * moment_one + (1.0 - beta_first) * clipped
    second_moment = beta_second * moment_two + (1.0 - beta_second) * clipped * clipped
    step_size = learn_rate / (1.0 - beta_first**adam_step)
    scaled = jnp.sqrt(second_moment / (1.0 - beta_second**adam_step)) + adam_eps
    return (table - step_size * first_moment / scaled, first_moment, second_moment)


def gather_sum(pieces, offsets, order, wide, narrow):
    arrived = [send(pieces[k], wide, narrow, offsets[k]) for k in order]
    out = pieces[0].astype(jnp.float32)
    for piece in arrived:
        out = out + piece.astype(jnp.float32)
    return out


def on_device(tokens, cotangent, lengths, item_rows, w_in, w_out, table, moment_one, moment_two):
    wide, narrow = lax.axis_size("wide"), lax.axis_size("narrow")
    rows_dev, width = table.shape
    cores, inner, pairs, outer = layout_of(wide, narrow)
    held = local_rows(wide, narrow, rows_dev, tokens, cotangent, lengths, item_rows, w_in, w_out)
    plane = inner * pairs
    stages = (
        ([(c, 0, 0, 0) for c in range(cores)], range(1, cores)),
        ([(0, i, y, 0) for i in range(inner) for y in range(pairs)], [plane - 1, *range(1, plane - 1)]),
        ([(0, 0, 0, z) for z in range(outer)], [1, *range(outer - 1, 1, -1)] if outer > 1 else []),
    )
    for number, (offsets, order) in enumerate(stages):
        if number:
            held = held.astype(jnp.bfloat16).reshape(len(offsets), -1, width)
        held = gather_sum(held, offsets, order, wide, narrow)
    return adam_rows(held, table, moment_one, moment_two)


def solution(mesh):
    return jax.shard_map(
        on_device,
        mesh=mesh,
        in_specs=(
            P(AXES, None, None),
            P(AXES, None, None),
            P(AXES),
            P(AXES, None),
            P(),
            P(),
            P(AXES, None),
            P(AXES, None),
            P(AXES, None),
        ),
        out_specs=(P(AXES, None), P(AXES, None), P(AXES, None)),
        check_vma=False,
    )
```

```python
import functools

import jax
import jax.numpy as jnp
from jax import lax
from jax.experimental import pallas as pl
from jax.experimental.pallas import tpu as pltpu
from jax.sharding import PartitionSpec as P

HEADS = 8
CORES = 2
LANES = 128

norm_eps = 1e-06
clip_norm = 4.0
learn_rate = 0.5
beta_first = 0.9
beta_second = 0.999
adam_step = 3.0
adam_eps = 1e-08

AXES = ("wide", "narrow")


def layout_of(wide, narrow):
    cores = CORES
    inner = 2 if wide % 2 == 0 else 1
    return cores, inner, narrow // cores, wide // inner


def shifted(at, by, size):
    return at ^ by if size & (size - 1) == 0 else (at + by) % size


def destination(wide, narrow, w, n, cr, ir, yr, zr):
    cores, inner, pairs, outer = layout_of(wide, narrow)
    z, i = w // inner, w % inner
    y, c = n // cores, n % cores
    w_to = shifted(z, zr, outer) * inner + shifted(i, ir, inner)
    n_to = shifted(y, yr, pairs) * cores + shifted(c, cr, cores)
    return w_to, n_to


def send(x, wide, narrow, offset):
    perm = []
    for w in range(wide):
        for n in range(narrow):
            w_to, n_to = destination(wide, narrow, w, n, *offset)
            perm.append((w * narrow + n, w_to * narrow + n_to))
    return lax.ppermute(x, AXES, perm)


def dot(a, b):
    return lax.dot_general(a, b, (((1,), (0,)), ((), ())), preferred_element_type=jnp.float32)


def dot_nt(a, b):
    return lax.dot_general(a, b, (((1,), (1,)), ((), ())), preferred_element_type=jnp.float32)


def local_kernel(
    wide, narrow, rows_dev,
    len_hbm, rows_hbm, tok_hbm, cot_hbm, win_hbm, wout_hbm,
    keep_ref, send_ref,
    len_ref, rows_ref, tok, cot, win, wout, hid, slope, att, fac, mixed, inner_grad, dgated, grads, dm_s, sems,
):
    micro, lmax, width = tok_hbm.shape
    half = lmax // 2
    per_head = width // HEADS
    f32, bf16 = jnp.float32, jnp.bfloat16
    total = micro * lmax
    bounds = (0, width, 2 * width, 4 * width)
    moves = [(tok_hbm, tok)]
    moves += [(win_hbm.at[:, lo:hi], win.at[:, lo:hi]) for lo, hi in zip(bounds, bounds[1:])]
    moves += [(wout_hbm, wout), (cot_hbm, cot), (len_hbm, len_ref), (rows_hbm, rows_ref)]
    copies = [pltpu.make_async_copy(src, dst, sems.at[i]) for i, (src, dst) in enumerate(moves)]
    for copy in copies:
        copy.start()

    tile = 256
    row = lax.broadcasted_iota(jnp.int32, (lmax, 1), 0)
    copies[0].wait()
    source = tok[...].reshape(total, width) * jnp.asarray(0.5, bf16)

    def activate(u, cols):
        th = jnp.tanh(u)
        up = 1.0 + th
        act = u * up
        hid[:, cols] = act.astype(bf16)
        slope[:, cols] = up + act * (1.0 - th)

    waiting = ()
    for part, (lo, hi) in enumerate(zip(bounds, bounds[1:])):
        copies[1 + part].wait()
        if hi == 4 * width:
            for copy in copies[len(bounds) :]:
                copy.wait()
            for s in range(micro):
                live = (row < len_ref[s]).astype(f32)
                cot[s] = (cot[s].astype(f32) * live).astype(bf16)
        for first in range(lo, hi, tile):
            cols = pl.ds(first, tile)
            u = dot(source, win[:, cols])
            if waiting:
                activate(*waiting)
            waiting = (u, cols)
    dgated[...] = dot_nt(cot[...].reshape(total, width), wout[...])
    activate(*waiting)

    lane = lax.broadcasted_iota(jnp.int32, (1, LANES), 1)
    heads_here = LANES // per_head
    masks = [((lane // per_head) == h).astype(bf16) for h in range(heads_here)]
    scale = per_head ** (-0.5)
    causal = lax.broadcasted_iota(jnp.int32, (half, half), 1) <= lax.broadcasted_iota(jnp.int32, (half, half), 0)
    none = jnp.zeros((half, half), bf16)
    far = -1e4
    lane_pairs = width // LANES
    group = 32
    groups = lmax // group

    def pick_lanes(stacked):
        out = stacked[:lmax]
        for h in range(1, heads_here):
            out = jnp.where(lane // per_head == h, stacked[h * lmax : (h + 1) * lmax], out)
        return out

    def forward_pair(s, p):
        here = pl.ds(s * lmax, lmax)
        q = hid[here, pl.ds(2 * width + p * LANES, LANES)]
        k = hid[here, pl.ds(3 * width + p * LANES, LANES)]
        v = hid[here, pl.ds(width + p * LANES, LANES)]
        qs = jnp.concatenate([q * (m * jnp.asarray(0.5 * scale, bf16)) for m in masks], axis=0)
        scores = dot_nt(qs, k)
        weights = []
        for h in range(heads_here):
            head = p * heads_here + h
            parts = []
            for b in range(2):
                rows = slice(b * half, (b + 1) * half)
                first = h * lmax + b * half
                pieces = []
                for c in range(b + 1):
                    cols = slice(c * half, (c + 1) * half)
                    u = scores[first : first + half, cols]
                    if c == b:
                        u = jnp.where(causal, u, far)
                    th = jnp.tanh(u)
                    up = 1.0 + th
                    act = u * up
                    fac[s, head, rows, cols] = up + act * (1.0 - th)
                    pieces.append(act.astype(bf16))
                if b == 0:
                    pieces.append(none)
                parts.append(jnp.concatenate(pieces, axis=1))
            weight = jnp.concatenate(parts, axis=0)
            att[s, head] = weight
            weights.append(weight)
        mixed[s, :, pl.ds(p * LANES, LANES)] = pick_lanes(dot(jnp.concatenate(weights, axis=0), v))

    def norm_group(s, r):
        rows = pl.ds(r * group, group)
        those = pl.ds(s * lmax + r * group, group)
        length = len_ref[s]
        place = lax.broadcasted_iota(jnp.int32, (group, 1), 0) + r * group
        share = jnp.where(place < length, 1.0 / jnp.full((group, 1), length, jnp.int32).astype(f32), 0.0)
        mix = mixed[s, rows, :] * share
        centered = mix - jnp.mean(mix, axis=1, keepdims=True)
        inv = lax.rsqrt(jnp.mean(centered * centered, axis=1, keepdims=True) + norm_eps)
        normed = centered * inv
        dg = dgated[those, :]
        gate = hid[those, pl.ds(0, width)].astype(f32)
        dgn = dg * normed
        inner_grad[those, pl.ds(0, width)] = (dgn * slope[those, pl.ds(0, width)]).astype(bf16)
        dn = dg * gate
        dmix = (inv * share) * (
            dn - jnp.mean(dn, axis=1, keepdims=True) - normed * jnp.mean(dgn * gate, axis=1, keepdims=True)
        )
        dm_s[s, rows, :] = dmix.astype(bf16)

    def backward_pair(s, p):
        here = pl.ds(s * lmax, lmax)
        lanes = pl.ds(p * LANES, LANES)
        q_t = hid[here, pl.ds(2 * width + p * LANES, LANES)].T
        k = hid[here, pl.ds(3 * width + p * LANES, LANES)]
        v = hid[here, pl.ds(width + p * LANES, LANES)]
        dmp = dm_s[s, :, lanes]
        dm_t = dmp.T
        small = jnp.asarray(0.5 * scale, bf16)
        d_att = dot_nt(jnp.concatenate([dmp * (m * small) for m in masks], axis=0), v)
        stacked, dks, dvs = [], [], []
        for h in range(heads_here):
            head = p * heads_here + h
            feat = slice(h * per_head, (h + 1) * per_head)
            dvs.append(dot(dm_t[feat], att[s, head]).astype(bf16))
            ds_top = (d_att[h * lmax : h * lmax + half, :half] * fac[s, head, :half, :half]).astype(bf16)
            ds_low = (d_att[h * lmax + half : (h + 1) * lmax] * fac[s, head, half:, :]).astype(bf16)
            ds = jnp.concatenate([jnp.concatenate([ds_top, none], axis=1), ds_low], axis=0)
            stacked.append(ds)
            dks.append(dot(q_t[feat], ds).astype(bf16))
        dv = jnp.concatenate(dvs, axis=0).T.astype(f32)
        dk = jnp.concatenate(dks, axis=0).T.astype(f32)
        dq = pick_lanes(dot(jnp.concatenate(stacked, axis=0), k))
        for part, piece in ((1, dv), (2, dq), (3, dk)):
            cols = pl.ds(part * width + p * LANES, LANES)
            inner_grad[here, cols] = (piece * slope[here, cols]).astype(bf16)

    each = -(-groups // lane_pairs)
    norm_chunks = [range(p * each, min((p + 1) * each, groups)) for p in range(lane_pairs)]
    for s in range(micro):
        for p in range(lane_pairs):
            forward_pair(s, p)
            if s > 0:
                for r in norm_chunks[p]:
                    norm_group(s - 1, r)
        if s > 0:
            for p in range(lane_pairs):
                backward_pair(s - 1, p)
                if s == micro - 1:
                    for r in norm_chunks[p]:
                        norm_group(s, r)
    if micro == 1:
        for r in range(groups):
            norm_group(0, r)
    for p in range(lane_pairs):
        backward_pair(micro - 1, p)

    back = 0.5 * dot_nt(inner_grad[...], win[...])
    grads[...] = (back + cot[...].reshape(total, width).astype(f32)).astype(bf16)

    cores, inner_w, pairs, outer = layout_of(wide, narrow)
    w_me, n_me = lax.axis_index("wide"), lax.axis_index("narrow")
    blocks = wide * narrow // cores
    per_chunk = min(8, blocks)
    size = per_chunk * rows_dev
    slot = lax.broadcasted_iota(jnp.int32, (rows_dev, lmax), 0)

    def fill(out_ref, core_offset):
        def one_chunk(j, carry):
            pieces = []
            for b in range(per_chunk):
                block = j * per_chunk + b
                zr = block % outer
                yr = (block // outer) % pairs
                ir = block // (outer * pairs)
                w_to, n_to = destination(wide, narrow, w_me, n_me, core_offset, ir, yr, zr)
                first = (w_to * narrow + n_to) * rows_dev
                pieces.append(
                    jnp.concatenate(
                        [(slot == rows_ref[s : s + 1, :] - first).astype(f32).astype(bf16) for s in range(micro)], axis=1
                    )
                )
            chosen = jnp.concatenate(pieces, axis=0)
            out_ref[pl.ds(pl.multiple_of(j * size, size), size), :] = dot(chosen, grads[...]).astype(bf16)
            return carry

        lax.fori_loop(0, blocks // per_chunk, one_chunk, 0, unroll=blocks // per_chunk <= 4)

    fill(send_ref, 1)
    fill(keep_ref, 0)


def local_rows(wide, narrow, rows_dev, tokens, cotangent, lengths, item_rows, w_in, w_out):
    micro, lmax, width = tokens.shape
    total = micro * lmax
    items = wide * narrow * rows_dev
    f32, bf16 = jnp.float32, jnp.bfloat16
    vmem = pl.BlockSpec(memory_space=pltpu.VMEM)
    hbm = pl.BlockSpec(memory_space=pltpu.HBM)
    part = jax.ShapeDtypeStruct((items // CORES, width), bf16)
    return pl.pallas_call(
        functools.partial(local_kernel, wide, narrow, rows_dev),
        out_shape=(part, part),
        in_specs=[hbm] * 6,
        out_specs=(vmem, vmem),
        scratch_shapes=[
            pltpu.SMEM((micro,), jnp.int32),
            pltpu.VMEM((micro, lmax), jnp.int32),
            pltpu.VMEM((micro, lmax, width), bf16),
            pltpu.VMEM((micro, lmax, width), bf16),
            pltpu.VMEM((width, 4 * width), bf16),
            pltpu.VMEM((width, width), bf16),
            pltpu.VMEM((total, 4 * width), bf16),
            pltpu.VMEM((total, 4 * width), f32),
            pltpu.VMEM((micro, HEADS, lmax, lmax), bf16),
            pltpu.VMEM((micro, HEADS, lmax, lmax), f32),
            pltpu.VMEM((micro, lmax, width), f32),
            pltpu.VMEM((total, 4 * width), bf16),
            pltpu.VMEM((total, width), f32),
            pltpu.VMEM((total, width), bf16),
            pltpu.VMEM((micro, lmax, width), bf16),
            pltpu.SemaphoreType.DMA((8,)),
        ],
        compiler_params=pltpu.CompilerParams(vmem_limit_bytes=(28 << 20) + 4 * items * width),
        cost_estimate=pl.CostEstimate(
            flops=16 * total * width * width + 12 * total * lmax * width,
            bytes_accessed=4 * total * width + 10 * width * width + 2 * items * width,
            transcendentals=HEADS * total * lmax,
        ),
        name="local_rows",
    )(*(pltpu.with_memory_space_constraint(a, pltpu.HBM) for a in (lengths, item_rows, tokens, cotangent, w_in, w_out)))


def adam_rows(row_grad, table, moment_one, moment_two):
    row_norms = jnp.sqrt(jnp.sum(row_grad * row_grad, axis=1, keepdims=True))
    clipped = row_grad * (clip_norm / jnp.maximum(row_norms, clip_norm))
    first_moment = beta_first * moment_one + (1.0 - beta_first) * clipped
    second_moment = beta_second * moment_two + (1.0 - beta_second) * clipped * clipped
    step_size = learn_rate / (1.0 - beta_first**adam_step)
    scaled = jnp.sqrt(second_moment / (1.0 - beta_second**adam_step)) + adam_eps
    return (table - step_size * first_moment / scaled, first_moment, second_moment)


def gather_sum(pieces, offsets, order, wide, narrow):
    arrived = [send(pieces[k], wide, narrow, offsets[k]) for k in order]
    out = pieces[0].astype(jnp.float32)
    for piece in arrived:
        out = out + piece.astype(jnp.float32)
    return out


def on_device(tokens, cotangent, lengths, item_rows, w_in, w_out, table, moment_one, moment_two):
    wide, narrow = lax.axis_size("wide"), lax.axis_size("narrow")
    rows_dev, width = table.shape
    cores, inner, pairs, outer = layout_of(wide, narrow)
    blocks = local_rows(wide, narrow, rows_dev, tokens, cotangent, lengths, item_rows, w_in, w_out)
    held = gather_sum(blocks, [(c, 0, 0, 0) for c in range(cores)], range(1, cores), wide, narrow)
    held = held.astype(jnp.bfloat16).reshape(inner * pairs, outer, rows_dev, width)
    plane = [(0, i, y, 0) for i in range(inner) for y in range(pairs)]
    cut = outer // 2
    summed = {}
    for lo, hi in ((cut, outer), (0, cut)):
        pieces = [held[k, lo:hi].reshape(-1, width) for k in range(len(plane))]
        part = gather_sum(pieces, plane, range(1, len(plane)), wide, narrow).reshape(hi - lo, rows_dev, width)
        summed.update({z: part[z - lo] for z in range(lo, hi)})
    order = [*range(cut, outer), *range(cut - 1, 0, -1)]
    pieces = [summed[z].astype(jnp.bfloat16) if z else summed[z] for z in range(outer)]
    held = gather_sum(pieces, [(0, 0, 0, z) for z in range(outer)], order, wide, narrow)
    return adam_rows(held, table, moment_one, moment_two)


def solution(mesh):
    return jax.shard_map(
        on_device,
        mesh=mesh,
        in_specs=(
            P(AXES, None, None),
            P(AXES, None, None),
            P(AXES),
            P(AXES, None),
            P(),
            P(),
            P(AXES, None),
            P(AXES, None),
            P(AXES, None),
        ),
        out_specs=(P(AXES, None), P(AXES, None), P(AXES, None)),
        check_vma=False,
    )
```

```python
import functools

import jax
import jax.numpy as jnp
from jax import lax
from jax.experimental import pallas as pl
from jax.experimental.pallas import tpu as pltpu
from jax.sharding import PartitionSpec as P

HEADS = 8
CORES = 2
LANES = 128

norm_eps = 1e-06
clip_norm = 4.0
learn_rate = 0.5
beta_first = 0.9
beta_second = 0.999
adam_step = 3.0
adam_eps = 1e-08

AXES = ("wide", "narrow")


def layout_of(wide, narrow):
    cores = CORES
    inner = 2 if wide % 2 == 0 else 1
    return cores, inner, narrow // cores, wide // inner


def shifted(at, by, size):
    return at ^ by if size & (size - 1) == 0 else (at + by) % size


def destination(wide, narrow, w, n, cr, ir, yr, zr):
    cores, inner, pairs, outer = layout_of(wide, narrow)
    z, i = w // inner, w % inner
    y, c = n // cores, n % cores
    w_to = shifted(z, zr, outer) * inner + shifted(i, ir, inner)
    n_to = shifted(y, yr, pairs) * cores + shifted(c, cr, cores)
    return w_to, n_to


def send(x, wide, narrow, offset):
    perm = []
    for w in range(wide):
        for n in range(narrow):
            w_to, n_to = destination(wide, narrow, w, n, *offset)
            perm.append((w * narrow + n, w_to * narrow + n_to))
    return lax.ppermute(x, AXES, perm)


def dot(a, b):
    return lax.dot_general(a, b, (((1,), (0,)), ((), ())), preferred_element_type=jnp.float32)


def dot_nt(a, b):
    return lax.dot_general(a, b, (((1,), (1,)), ((), ())), preferred_element_type=jnp.float32)


def local_kernel(
    wide, narrow, rows_dev,
    len_hbm, rows_hbm, tok_hbm, cot_hbm, win_hbm, wout_hbm,
    keep_ref, send_ref,
    len_ref, rows_ref, tok, cot, win, wout, hid, slope, att, fac, mixed, inner_grad, dgated, grads, dm_s, sems,
):
    micro, lmax, width = tok_hbm.shape
    half = lmax // 2
    per_head = width // HEADS
    f32, bf16 = jnp.float32, jnp.bfloat16
    total = micro * lmax
    bounds = (0, width, 2 * width, 4 * width)
    moves = [(tok_hbm, tok)]
    moves += [(win_hbm.at[:, lo:hi], win.at[:, lo:hi]) for lo, hi in zip(bounds, bounds[1:])]
    moves += [(wout_hbm, wout), (cot_hbm, cot), (len_hbm, len_ref), (rows_hbm, rows_ref)]
    copies = [pltpu.make_async_copy(src, dst, sems.at[i]) for i, (src, dst) in enumerate(moves)]
    for copy in copies:
        copy.start()

    tile = 256
    row = lax.broadcasted_iota(jnp.int32, (lmax, 1), 0)
    copies[0].wait()
    source = tok[...].reshape(total, width) * jnp.asarray(0.5, bf16)

    def activate(u, rows, cols):
        th = jnp.tanh(u)
        up = 1.0 + th
        act = u * up
        hid[rows, cols] = act.astype(bf16)
        slope[rows, cols] = up + act * (1.0 - th)

    waiting = ()
    for part, (lo, hi) in enumerate(zip(bounds, bounds[1:])):
        copies[1 + part].wait()
        if hi == 4 * width:
            for copy in copies[len(bounds) :]:
                copy.wait()
            for s in range(micro):
                live = (row < len_ref[s]).astype(f32)
                cot[s] = (cot[s].astype(f32) * live).astype(bf16)
        for first in range(lo, hi, tile):
            cols = pl.ds(first, tile)
            for top in range(0, total, lmax):
                u = dot(source[top : top + lmax], win[:, cols])
                if waiting:
                    activate(*waiting)
                waiting = (u, pl.ds(top, lmax), cols)
    dgated[...] = dot_nt(cot[...].reshape(total, width), wout[...])
    activate(*waiting)

    lane = lax.broadcasted_iota(jnp.int32, (1, LANES), 1)
    heads_here = LANES // per_head
    masks = [((lane // per_head) == h).astype(bf16) for h in range(heads_here)]
    scale = per_head ** (-0.5)
    causal = lax.broadcasted_iota(jnp.int32, (half, half), 1) <= lax.broadcasted_iota(jnp.int32, (half, half), 0)
    none = jnp.zeros((half, half), bf16)
    far = -1e4
    lane_pairs = width // LANES
    group = 32
    groups = lmax // group

    def pick_lanes(stacked):
        out = stacked[:lmax]
        for h in range(1, heads_here):
            out = jnp.where(lane // per_head == h, stacked[h * lmax : (h + 1) * lmax], out)
        return out

    def forward_pair(s, p):
        here = pl.ds(s * lmax, lmax)
        q = hid[here, pl.ds(2 * width + p * LANES, LANES)]
        k = hid[here, pl.ds(3 * width + p * LANES, LANES)]
        v = hid[here, pl.ds(width + p * LANES, LANES)]
        qs = jnp.concatenate([q * (m * jnp.asarray(0.5 * scale, bf16)) for m in masks], axis=0)
        scores = dot_nt(qs, k)
        weights = []
        for h in range(heads_here):
            head = p * heads_here + h
            parts = []
            for b in range(2):
                rows = slice(b * half, (b + 1) * half)
                first = h * lmax + b * half
                pieces = []
                for c in range(b + 1):
                    cols = slice(c * half, (c + 1) * half)
                    u = scores[first : first + half, cols]
                    if c == b:
                        u = jnp.where(causal, u, far)
                    th = jnp.tanh(u)
                    up = 1.0 + th
                    act = u * up
                    fac[s, head, rows, cols] = up + act * (1.0 - th)
                    pieces.append(act.astype(bf16))
                if b == 0:
                    pieces.append(none)
                parts.append(jnp.concatenate(pieces, axis=1))
            weight = jnp.concatenate(parts, axis=0)
            att[s, head] = weight
            weights.append(weight)
        mixed[s, :, pl.ds(p * LANES, LANES)] = pick_lanes(dot(jnp.concatenate(weights, axis=0), v))

    def norm_group(s, r):
        rows = pl.ds(r * group, group)
        those = pl.ds(s * lmax + r * group, group)
        length = len_ref[s]
        place = lax.broadcasted_iota(jnp.int32, (group, 1), 0) + r * group
        share = jnp.where(place < length, 1.0 / jnp.full((group, 1), length, jnp.int32).astype(f32), 0.0)
        mix = mixed[s, rows, :] * share
        centered = mix - jnp.mean(mix, axis=1, keepdims=True)
        inv = lax.rsqrt(jnp.mean(centered * centered, axis=1, keepdims=True) + norm_eps)
        normed = centered * inv
        dg = dgated[those, :]
        gate = hid[those, pl.ds(0, width)].astype(f32)
        dgn = dg * normed
        inner_grad[those, pl.ds(0, width)] = (dgn * slope[those, pl.ds(0, width)]).astype(bf16)
        dn = dg * gate
        dmix = (inv * share) * (
            dn - jnp.mean(dn, axis=1, keepdims=True) - normed * jnp.mean(dgn * gate, axis=1, keepdims=True)
        )
        dm_s[s, rows, :] = dmix.astype(bf16)

    def backward_pair(s, p):
        here = pl.ds(s * lmax, lmax)
        lanes = pl.ds(p * LANES, LANES)
        q_t = hid[here, pl.ds(2 * width + p * LANES, LANES)].T
        k = hid[here, pl.ds(3 * width + p * LANES, LANES)]
        v = hid[here, pl.ds(width + p * LANES, LANES)]
        dmp = dm_s[s, :, lanes]
        dm_t = dmp.T
        small = jnp.asarray(0.5 * scale, bf16)
        d_att = dot_nt(jnp.concatenate([dmp * (m * small) for m in masks], axis=0), v)
        stacked, dks, dvs = [], [], []
        for h in range(heads_here):
            head = p * heads_here + h
            feat = slice(h * per_head, (h + 1) * per_head)
            dvs.append(dot(dm_t[feat], att[s, head]).astype(bf16))
            ds_top = (d_att[h * lmax : h * lmax + half, :half] * fac[s, head, :half, :half]).astype(bf16)
            ds_low = (d_att[h * lmax + half : (h + 1) * lmax] * fac[s, head, half:, :]).astype(bf16)
            ds = jnp.concatenate([jnp.concatenate([ds_top, none], axis=1), ds_low], axis=0)
            stacked.append(ds)
            dks.append(dot(q_t[feat], ds).astype(bf16))
        dv = jnp.concatenate(dvs, axis=0).T.astype(f32)
        dk = jnp.concatenate(dks, axis=0).T.astype(f32)
        dq = pick_lanes(dot(jnp.concatenate(stacked, axis=0), k))
        for part, piece in ((1, dv), (2, dq), (3, dk)):
            cols = pl.ds(part * width + p * LANES, LANES)
            inner_grad[here, cols] = (piece * slope[here, cols]).astype(bf16)

    each = -(-groups // lane_pairs)
    norm_chunks = [range(p * each, min((p + 1) * each, groups)) for p in range(lane_pairs)]
    for s in range(micro):
        for p in range(lane_pairs):
            forward_pair(s, p)
            if s > 0:
                for r in norm_chunks[p]:
                    norm_group(s - 1, r)
        if s > 0:
            for p in range(lane_pairs):
                backward_pair(s - 1, p)
                if s == micro - 1:
                    for r in norm_chunks[p]:
                        norm_group(s, r)
    if micro == 1:
        for r in range(groups):
            norm_group(0, r)
    for p in range(lane_pairs):
        backward_pair(micro - 1, p)

    back = 0.5 * dot_nt(inner_grad[...], win[...])
    grads[...] = (back + cot[...].reshape(total, width).astype(f32)).astype(bf16)

    cores, inner_w, pairs, outer = layout_of(wide, narrow)
    w_me, n_me = lax.axis_index("wide"), lax.axis_index("narrow")
    blocks = wide * narrow // cores
    per_chunk = min(8, blocks)
    size = per_chunk * rows_dev
    slot = lax.broadcasted_iota(jnp.int32, (rows_dev, lmax), 0)

    def fill(out_ref, core_offset):
        def one_chunk(j, carry):
            pieces = []
            for b in range(per_chunk):
                block = j * per_chunk + b
                zr = block % outer
                yr = (block // outer) % pairs
                ir = block // (outer * pairs)
                w_to, n_to = destination(wide, narrow, w_me, n_me, core_offset, ir, yr, zr)
                first = (w_to * narrow + n_to) * rows_dev
                pieces.append(
                    jnp.concatenate(
                        [(slot == rows_ref[s : s + 1, :] - first).astype(f32).astype(bf16) for s in range(micro)], axis=1
                    )
                )
            chosen = jnp.concatenate(pieces, axis=0)
            out_ref[pl.ds(pl.multiple_of(j * size, size), size), :] = dot(chosen, grads[...]).astype(bf16)
            return carry

        lax.fori_loop(0, blocks // per_chunk, one_chunk, 0, unroll=blocks // per_chunk <= 4)

    fill(send_ref, 1)
    fill(keep_ref, 0)


def local_rows(wide, narrow, rows_dev, tokens, cotangent, lengths, item_rows, w_in, w_out):
    micro, lmax, width = tokens.shape
    total = micro * lmax
    items = wide * narrow * rows_dev
    f32, bf16 = jnp.float32, jnp.bfloat16
    vmem = pl.BlockSpec(memory_space=pltpu.VMEM)
    hbm = pl.BlockSpec(memory_space=pltpu.HBM)
    part = jax.ShapeDtypeStruct((items // CORES, width), bf16)
    return pl.pallas_call(
        functools.partial(local_kernel, wide, narrow, rows_dev),
        out_shape=(part, part),
        in_specs=[hbm] * 6,
        out_specs=(vmem, vmem),
        scratch_shapes=[
            pltpu.SMEM((micro,), jnp.int32),
            pltpu.VMEM((micro, lmax), jnp.int32),
            pltpu.VMEM((micro, lmax, width), bf16),
            pltpu.VMEM((micro, lmax, width), bf16),
            pltpu.VMEM((width, 4 * width), bf16),
            pltpu.VMEM((width, width), bf16),
            pltpu.VMEM((total, 4 * width), bf16),
            pltpu.VMEM((total, 4 * width), f32),
            pltpu.VMEM((micro, HEADS, lmax, lmax), bf16),
            pltpu.VMEM((micro, HEADS, lmax, lmax), f32),
            pltpu.VMEM((micro, lmax, width), f32),
            pltpu.VMEM((total, 4 * width), bf16),
            pltpu.VMEM((total, width), f32),
            pltpu.VMEM((total, width), bf16),
            pltpu.VMEM((micro, lmax, width), bf16),
            pltpu.SemaphoreType.DMA((8,)),
        ],
        compiler_params=pltpu.CompilerParams(vmem_limit_bytes=(28 << 20) + 4 * items * width),
        cost_estimate=pl.CostEstimate(
            flops=16 * total * width * width + 12 * total * lmax * width,
            bytes_accessed=4 * total * width + 10 * width * width + 2 * items * width,
            transcendentals=HEADS * total * lmax,
        ),
        name="local_rows",
    )(*(pltpu.with_memory_space_constraint(a, pltpu.HBM) for a in (lengths, item_rows, tokens, cotangent, w_in, w_out)))


def adam_rows(row_grad, table, moment_one, moment_two):
    row_norms = jnp.sqrt(jnp.sum(row_grad * row_grad, axis=1, keepdims=True))
    clipped = row_grad * (clip_norm / jnp.maximum(row_norms, clip_norm))
    first_moment = beta_first * moment_one + (1.0 - beta_first) * clipped
    second_moment = beta_second * moment_two + (1.0 - beta_second) * clipped * clipped
    step_size = learn_rate / (1.0 - beta_first**adam_step)
    scaled = jnp.sqrt(second_moment / (1.0 - beta_second**adam_step)) + adam_eps
    return (table - step_size * first_moment / scaled, first_moment, second_moment)


def gather_sum(pieces, offsets, order, wide, narrow):
    arrived = [send(pieces[k], wide, narrow, offsets[k]) for k in order]
    out = pieces[0].astype(jnp.float32)
    for piece in arrived:
        out = out + piece.astype(jnp.float32)
    return out


def on_device(tokens, cotangent, lengths, item_rows, w_in, w_out, table, moment_one, moment_two):
    wide, narrow = lax.axis_size("wide"), lax.axis_size("narrow")
    rows_dev, width = table.shape
    cores, inner, pairs, outer = layout_of(wide, narrow)
    blocks = local_rows(wide, narrow, rows_dev, tokens, cotangent, lengths, item_rows, w_in, w_out)
    held = gather_sum(blocks, [(c, 0, 0, 0) for c in range(cores)], range(1, cores), wide, narrow)
    held = held.astype(jnp.bfloat16).reshape(inner * pairs, outer, rows_dev, width)
    plane = [(0, i, y, 0) for i in range(inner) for y in range(pairs)]
    cut = outer // 2
    summed = {}
    for lo, hi in ((cut, outer), (0, cut)):
        pieces = [held[k, lo:hi].reshape(-1, width) for k in range(len(plane))]
        part = gather_sum(pieces, plane, range(1, len(plane)), wide, narrow).reshape(hi - lo, rows_dev, width)
        summed.update({z: part[z - lo] for z in range(lo, hi)})
    order = [*range(cut, outer), *range(cut - 1, 0, -1)]
    pieces = [summed[z].astype(jnp.bfloat16) if z else summed[z] for z in range(outer)]
    held = gather_sum(pieces, [(0, 0, 0, z) for z in range(outer)], order, wide, narrow)
    return adam_rows(held, table, moment_one, moment_two)


def solution(mesh):
    return jax.shard_map(
        on_device,
        mesh=mesh,
        in_specs=(
            P(AXES, None, None),
            P(AXES, None, None),
            P(AXES),
            P(AXES, None),
            P(),
            P(),
            P(AXES, None),
            P(AXES, None),
            P(AXES, None),
        ),
        out_specs=(P(AXES, None), P(AXES, None), P(AXES, None)),
        check_vma=False,
    )
```
